8 devices in a mesh: dp: 1 (over z), a: 2 (over y), b: 4 (over x, core).
Axes of the slice: x: 2, y: 2, z: 1, core: 2. Of those that a mesh axis runs over, the one named last changes fastest.
Arguments:
- x: bfloat16 [2048, 8192], P('dp', ('a', 'b'))
- w_gate: bfloat16 [8192, 28672], P('a', 'b')
- w_up: bfloat16 [8192, 28672], P('a', 'b')
- w_down: bfloat16 [28672, 8192], P('b', 'a')
Outputs:
- output: bfloat16 [2048, 8192], P('dp', ('a', 'b'))
All inputs are finite; a program needn't handle non-finite values.
Results may differ from the reference program's by a relative error of at most 0.016.
Values are sent between devices in bfloat16 or wider.
A program may use at most 2 GiB of HBM per device.

```python
import jax
import jax.numpy as jnp

ROWS = 2048
D = 8192
FF = 28672


def setup_inputs(seed: int = 0, part: int = 0) -> dict:
    kx, kg, ku, kd = jax.random.split(jax.random.key(seed), 4)
    drawn = {
        "x": jax.random.normal(jax.random.fold_in(kx, part), (ROWS, D), jnp.float32),
        "w_gate": jax.random.normal(kg, (D, FF), jnp.float32) * D**-0.5,
        "w_up": jax.random.normal(ku, (D, FF), jnp.float32) * D**-0.5,
        "w_down": jax.random.normal(kd, (FF, D), jnp.float32) * FF**-0.5,
    }
    return {k: v.astype(jnp.bfloat16) for k, v in drawn.items()}


def reference(x, w_gate, w_up, w_down):
    gate = jnp.dot(x, w_gate, preferred_element_type=jnp.float32)
    up = jnp.dot(x, w_up, preferred_element_type=jnp.float32)
    hidden = (jax.nn.silu(gate) * up).astype(jnp.bfloat16)
    return jnp.dot(hidden, w_down, preferred_element_type=jnp.float32).astype(jnp.bfloat16)
```

```python
import jax
import jax.numpy as jnp
from jax import lax
from jax.experimental import pallas as pl
from jax.experimental.pallas import tpu as pltpu
from jax.sharding import PartitionSpec as P

MESH = pl.DeviceIdType.MESH
M = 128
TN = 512
SUB = 256


def _kernel(x_hbm, wg_hbm, wu_hbm, wd_hbm, y_hbm,
            xg, wring, stage, recv, hid, ystage, yrecv, yown, yout,
            wsem, xlsem, xssem, xrsem, pssem, prsem, hssem, hrsem, yssem, yrsem, yosem):
    f32, bf16 = jnp.float32, jnp.bfloat16
    rows, xcols = x_hbm.shape
    depth, ff = wg_hbm.shape
    dcols = wd_hbm.shape[1]
    half = ff // 2
    steps = rows // (2 * M)
    nt = ff // TN
    nd = dcols // TN
    per = xcols // TN

    dp = lax.axis_index("dp")
    a = lax.axis_index("a")
    b = lax.axis_index("b")
    chip, core = b // 2, b % 2
    peer = (dp, 1 - a, b)

    def mate(q):
        fx = 1 - q // 2
        fc = ((q + 1) // 2) % 2
        return 2 * (chip + fx - 2 * chip * fx) + core + fc - 2 * core * fc

    def w_copies(kind, i, slot):
        if kind == "gu":
            cols = pl.ds(pl.multiple_of(i * TN, TN), TN)
            return [pltpu.make_async_copy(w.at[:, cols], wring.at[slot, k], wsem.at[slot, k])
                    for k, w in enumerate((wg_hbm, wu_hbm))]
        cols = pl.ds(pl.multiple_of(mate(i // per) * xcols + (i % per) * TN, TN), TN)
        return [pltpu.make_async_copy(wd_hbm.at[pl.ds(k * half, half), cols],
                                      wring.at[slot, k, pl.ds(0, half)], wsem.at[slot, k])
                for k in range(2)]

    def w_start(kind, i, slot):
        for c in w_copies(kind, i, slot):
            c.start()

    def w_wait(kind, i, slot):
        for c in w_copies(kind, i, slot):
            c.wait()

    def x_rows(c):
        s, mine = c // 2, c % 2
        src = s * 2 * M + (a * mine + (1 - a) * (1 - mine)) * M
        return pl.ds(pl.multiple_of(src, M), M), pl.ds(pl.multiple_of(c * M, M), M)

    def x_local(c):
        src, dst = x_rows(c)
        return pltpu.make_async_copy(
            x_hbm.at[src], xg.at[dst, pl.ds(pl.multiple_of(b * xcols, xcols), xcols)], xlsem.at[c])

    def x_remote(c, q):
        src, dst = x_rows(c)
        return pltpu.make_async_remote_copy(
            src_ref=x_hbm.at[src], dst_ref=xg.at[dst, pl.ds(pl.multiple_of(b * xcols, xcols), xcols)],
            send_sem=xssem.at[c, q], recv_sem=xrsem.at[c, q],
            device_id=(dp, a, mate(q)), device_id_type=MESH)

    def x_wait(c):
        x_local(c).wait()
        for q in range(3):
            x_remote(c, q).wait_recv()

    def p_copy(t, n):
        return pltpu.make_async_remote_copy(
            src_ref=stage.at[n], dst_ref=recv.at[t % 2, n], send_sem=pssem.at[n], recv_sem=prsem.at[t % 2, n],
            device_id=peer, device_id_type=MESH)

    def h_copy(s, n, place):
        ref = hid.at[s % 3, pl.ds(pl.multiple_of(place * M, M), M), pl.ds(pl.multiple_of(n * TN, TN), TN)]
        return pltpu.make_async_remote_copy(
            src_ref=ref, dst_ref=ref, send_sem=hssem.at[s % 3, n], recv_sem=hrsem.at[s % 3, n],
            device_id=peer, device_id_type=MESH)

    def tiles(t, do_p, do_o, last_next):
        lo = 2 * M * t - (M if do_o else 0)
        size = M * (int(do_p) + int(do_o))
        xrow = pl.ds(lo if isinstance(lo, int) else pl.multiple_of(lo, M), size)
        if do_o:
            x_wait(2 * t - 1)
        if do_p:
            x_wait(2 * t)

        def tile(n, carry):
            slot = n % 2
            w_wait("gu", n, slot)

            @pl.when(n < nt - 1)
            def _():
                w_start("gu", n + 1, 1 - slot)

            @pl.when(n == nt - 1)
            def _():
                last_next()

            if do_o:
                p_copy(t - 1, n).wait()
            for j in range(TN // SUB):
                cols = pl.ds(j * SUB, SUB)
                xv = xg[xrow, :]
                g = jnp.dot(xv, wring[slot, 0, :, cols], preferred_element_type=f32)
                u = jnp.dot(xv, wring[slot, 1, :, cols], preferred_element_type=f32)
                if do_p:
                    stage[n, pl.ds(0, M), cols] = g[size - M:].astype(bf16)
                    stage[n, pl.ds(M, M), cols] = u[size - M:].astype(bf16)
                if do_o:
                    og = g[:M] + recv[(t - 1) % 2, n, pl.ds(0, M), cols].astype(f32)
                    ou = u[:M] + recv[(t - 1) % 2, n, pl.ds(M, M), cols].astype(f32)
                    h = og * jax.nn.sigmoid(og) * ou
                    hid[(t - 1) % 3, pl.ds(pl.multiple_of(a * M, M), M),
                        pl.ds(pl.multiple_of(n * TN + j * SUB, SUB), SUB)] = h.astype(bf16)
            if do_p:
                p_copy(t, n).start()
            if do_o:
                h_copy(t - 1, n, a).start()
            return carry

        lax.fori_loop(0, nt, tile, 0)

    def y_copy(s, q, h):
        cols = pl.ds(pl.multiple_of(h * TN, TN), TN)
        return pltpu.make_async_remote_copy(
            src_ref=ystage.at[q, :, cols], dst_ref=yrecv.at[s % 2, q, :, cols],
            send_sem=yssem.at[q, h], recv_sem=yrsem.at[s % 2, q, h],
            device_id=(dp, a, mate(q)), device_id_type=MESH)

    def y_out(s):
        return pltpu.make_async_copy(
            yout, y_hbm.at[pl.ds(pl.multiple_of(s * 2 * M, 2 * M), 2 * M)], yosem)

    def finish(s, first):
        for q in range(3):
            for h in range(per):
                y_copy(s, q, h).wait()
        if first is not True:
            @pl.when(jnp.logical_not(first))
            def _():
                y_out(s - 1).wait()

        def chunk(i, carry):
            r = pl.ds(pl.multiple_of(i * 32, 32), 32)
            acc = yown[r, :]
            for q in range(3):
                acc = acc + yrecv[s % 2, q, r, :].astype(f32)
            yout[r, :] = acc.astype(bf16)
            return carry

        lax.fori_loop(0, 2 * M // 32, chunk, 0)
        y_out(s).start()

    def down(s, last_next):
        def arrived(n, carry):
            h_copy(s, n, 1 - a).wait_recv()
            h_copy(s, n, a).wait_send()
            return carry

        lax.fori_loop(0, nt, arrived, 0)

        def tile(i, carry):
            slot = i % 2
            q, h = i // per, i % per
            w_wait("d", i, slot)

            @pl.when(i < nd - 1)
            def _():
                w_start("d", i + 1, 1 - slot)

            @pl.when(i == nd - 1)
            def _():
                last_next()

            for j in range(TN // SUB):
                wc = pl.ds(j * SUB, SUB)
                out = jnp.dot(hid[s % 3, :, pl.ds(0, half)], wring[slot, 0, pl.ds(0, half), wc],
                              preferred_element_type=f32)
                out = out + jnp.dot(hid[s % 3, :, pl.ds(half, half)], wring[slot, 1, pl.ds(0, half), wc],
                                    preferred_element_type=f32)
                cols = pl.ds(pl.multiple_of(h * TN + j * SUB, SUB), SUB)

                @pl.when(q < 3)
                def _():
                    ystage[q, :, cols] = out.astype(bf16)

                @pl.when(q == 3)
                def _():
                    yown[:, cols] = out

            @pl.when(q < 3)
            def _():
                y_copy(s, q, h).start()

            return carry

        lax.fori_loop(0, nd, tile, 0)

    w_start("gu", 0, 0)
    for c in range(2 * steps):
        x_local(c).start()

    barrier = pltpu.get_barrier_semaphore()
    pl.semaphore_signal(barrier, inc=1, device_id=peer, device_id_type=MESH)
    for q in range(3):
        pl.semaphore_signal(barrier, inc=1, device_id=(dp, a, mate(q)), device_id_type=MESH)
    pl.semaphore_wait(barrier, 4)

    def send_x(c, carry):
        for q in range(3):
            x_remote(c, q).start()
        return carry

    lax.fori_loop(0, 2 * steps, send_x, 0)

    gu0 = lambda: w_start("gu", 0, 0)
    d0 = lambda: w_start("d", 0, 0)

    tiles(0, True, False, gu0)
    tiles(1, True, True, gu0)
    tiles(2, True, True, d0)
    down(0, gu0)

    def step(t, carry):
        tiles(t, True, True, d0)
        finish(t - 3, t == 3)
        down(t - 2, gu0)
        return carry

    lax.fori_loop(3, steps, step, 0)

    tiles(steps, False, True, d0)
    finish(steps - 3, steps == 3)
    down(steps - 2, d0)
    finish(steps - 2, False)
    down(steps - 1, lambda: None)
    finish(steps - 1, False)
    y_out(steps - 1).wait()

    def drain(c, carry):
        for q in range(3):
            x_remote(c, q).wait_send()
        return carry

    lax.fori_loop(0, 2 * steps, drain, 0)


def solution(mesh):
    def body(x, wg, wu, wd):
        rows, xcols = x.shape
        depth, ff = wg.shape
        dcols = wd.shape[1]
        steps, nt, per = rows // (2 * M), ff // TN, xcols // TN
        bf16 = jnp.bfloat16
        anyspace = pl.BlockSpec(memory_space=pl.ANY)
        dma = pltpu.SemaphoreType.DMA
        return pl.pallas_call(
            _kernel,
            out_shape=jax.ShapeDtypeStruct(x.shape, x.dtype),
            in_specs=[anyspace] * 4,
            out_specs=anyspace,
            scratch_shapes=[
                pltpu.VMEM((rows, depth), bf16),
                pltpu.VMEM((2, 2, depth, TN), bf16),
                pltpu.VMEM((nt, 2 * M, TN), bf16),
                pltpu.VMEM((2, nt, 2 * M, TN), bf16),
                pltpu.VMEM((3, 2 * M, ff), bf16),
                pltpu.VMEM((3, 2 * M, xcols), bf16),
                pltpu.VMEM((2, 3, 2 * M, xcols), bf16),
                pltpu.VMEM((2 * M, xcols), jnp.float32),
                pltpu.VMEM((2 * M, xcols), bf16),
                dma((2, 2)),
                dma((2 * steps,)),
                dma((2 * steps, 3)),
                dma((2 * steps, 3)),
                dma((nt,)),
                dma((2, nt)),
                dma((3, nt)),
                dma((3, nt)),
                dma((3, per)),
                dma((2, 3, per)),
                dma(()),
            ],
            compiler_params=pltpu.CompilerParams(
                collective_id=0, has_side_effects=True, vmem_limit_bytes=67043328),
        )(x, wg, wu, wd)

    return jax.shard_map(
        body, mesh=mesh,
        in_specs=(P("dp", ("a", "b")), P("a", "b"), P("a", "b"), P("b", "a")),
        out_specs=P("dp", ("a", "b")), check_vma=False)
```

```python
import jax
import jax.numpy as jnp
from jax import lax
from jax.experimental import pallas as pl
from jax.experimental.pallas import tpu as pltpu
from jax.sharding import PartitionSpec as P

MESH = pl.DeviceIdType.MESH
M = 128
HM = M // 2
TN = 512
SUB = 512


def _kernel(x_hbm, wg_hbm, wu_hbm, wd_hbm, y_hbm,
            xg, wring, stage, recv, hid, ystage, yrecv, ymate, yown, yout, acc,
            wsem, xlsem, xssem, xrsem, x0ssem, x0rsem, pssem, prsem, p0ssem, p0rsem, hssem, hrsem,
            yssem, yrsem, ymsem, yosem):
    f32, bf16 = jnp.float32, jnp.bfloat16
    rows, xcols = x_hbm.shape
    depth, ff = wg_hbm.shape
    dcols = wd_hbm.shape[1]
    half = ff // 2
    steps = rows // (2 * M)
    nt = ff // TN
    nd = dcols // TN
    per = xcols // TN

    dp = lax.axis_index("dp")
    a = lax.axis_index("a")
    b = lax.axis_index("b")
    chip, core = b // 2, b % 2
    peer = (dp, 1 - a, b)

    def mate(q):
        fx = 1 - q // 2
        fc = ((q + 1) // 2) % 2
        return 2 * (chip + fx - 2 * chip * fx) + core + fc - 2 * core * fc

    def d_tile(o):
        late = o // 4
        return (1 - late) * (1 - o % 2) + late * (o // 2), (1 - late) * (o // 2) + late * (o % 2)

    def w_copies(kind, i, slot):
        if kind == "gu":
            cols = pl.ds(pl.multiple_of(i * TN, TN), TN)
            return [pltpu.make_async_copy(w.at[:, cols], wring.at[slot, k], wsem.at[slot, k])
                    for k, w in enumerate((wg_hbm, wu_hbm))]
        out = []
        for k in range(2):
            q, h = d_tile(i if kind == "d" else 2 * i + k)
            part = {"d": k, "d0": 0, "d1": 1}[kind]
            cols = pl.ds(pl.multiple_of(mate(q) * xcols + h * TN, TN), TN)
            out.append(pltpu.make_async_copy(wd_hbm.at[pl.ds(part * half, half), cols],
                                             wring.at[slot, k, pl.ds(0, half)], wsem.at[slot, k]))
        return out

    def w_start(kind, i, slot):
        for c in w_copies(kind, i, slot):
            c.start()

    def w_wait(kind, i, slot):
        for c in w_copies(kind, i, slot):
            c.wait()

    def x_rows(c):
        s, mine = c // 2, c % 2
        src = s * 2 * M + (a * mine + (1 - a) * (1 - mine)) * M
        return pl.ds(pl.multiple_of(src, M), M), pl.ds(pl.multiple_of(c * M, M), M)

    def x_local(c):
        src, dst = x_rows(c)
        return pltpu.make_async_copy(
            x_hbm.at[src], xg.at[dst, pl.ds(pl.multiple_of(b * xcols, xcols), xcols)], xlsem.at[c])

    def x_remote(c, q):
        src, dst = x_rows(c)
        return pltpu.make_async_remote_copy(
            src_ref=x_hbm.at[src], dst_ref=xg.at[dst, pl.ds(pl.multiple_of(b * xcols, xcols), xcols)],
            send_sem=xssem.at[c, q], recv_sem=xrsem.at[c, q],
            device_id=(dp, a, mate(q)), device_id_type=MESH)

    def x_wait(c):
        x_local(c).wait()
        for q in range(3):
            x_remote(c, q).wait_recv()

    def x_first(k, q):
        src = pl.ds(pl.multiple_of((1 - a) * M + k * HM, HM), HM)
        dst = pl.ds(k * HM, HM)
        if q < 2:
            cols = pl.ds(pl.multiple_of(b * xcols, xcols), xcols)
            source = x_hbm.at[src]
        else:
            cols = pl.ds(pl.multiple_of(mate(0) * xcols, xcols), xcols)
            source = xg.at[dst, cols]
        return pltpu.make_async_remote_copy(
            src_ref=source, dst_ref=xg.at[dst, cols], send_sem=x0ssem.at[q, k], recv_sem=x0rsem.at[q, k],
            device_id=(dp, a, mate(0 if q == 0 else 2)), device_id_type=MESH)

    def p_first(n, k):
        ref = pl.ds(k * M, M)
        return pltpu.make_async_remote_copy(
            src_ref=stage.at[n, ref], dst_ref=recv.at[0, n, ref], send_sem=p0ssem.at[n, k], recv_sem=p0rsem.at[n, k],
            device_id=peer, device_id_type=MESH)

    def first(last_next):
        def tile(n, carry):
            slot = n % 2
            w_wait("gu", n, slot)

            @pl.when(n < nt - 1)
            def _():
                w_start("gu", n + 1, 1 - slot)

            @pl.when(n == nt - 1)
            def _():
                last_next()

            for k in range(2):
                @pl.when(n == 0)
                def _():
                    if k == 0:
                        x_local(0).wait()
                    x_first(k, 0).wait_recv()
                    x_first(k, 2).start()
                    x_first(k, 1).wait_recv()
                    x_first(k, 2).wait_recv()

                for j in range(TN // SUB):
                    cols = pl.ds(j * SUB, SUB)
                    xv = xg[pl.ds(k * HM, HM), :]
                    g = jnp.dot(xv, wring[slot, 0, :, cols], preferred_element_type=f32)
                    u = jnp.dot(xv, wring[slot, 1, :, cols], preferred_element_type=f32)
                    stage[n, pl.ds(k * M, HM), cols] = g.astype(bf16)
                    stage[n, pl.ds(k * M + HM, HM), cols] = u.astype(bf16)
                p_first(n, k).start()

            for q in range(3):
                x_remote(n + 1, q).start()
            return carry

        lax.fori_loop(0, nt, tile, 0)
        for c in range(nt + 1, 2 * steps):
            for q in range(3):
                x_remote(c, q).start()

    def p_copy(t, n):
        return pltpu.make_async_remote_copy(
            src_ref=stage.at[n], dst_ref=recv.at[t % 2, n], send_sem=pssem.at[n], recv_sem=prsem.at[t % 2, n],
            device_id=peer, device_id_type=MESH)

    def h_copy(s, n, place):
        ref = hid.at[s % 3, pl.ds(pl.multiple_of(place * M, M), M), pl.ds(pl.multiple_of(n * TN, TN), TN)]
        return pltpu.make_async_remote_copy(
            src_ref=ref, dst_ref=ref, send_sem=hssem.at[s % 3, n], recv_sem=hrsem.at[s % 3, n],
            device_id=peer, device_id_type=MESH)

    def tiles(t, do_p, last_next):
        lo = 2 * M * t - M
        xrow = pl.ds(lo if isinstance(lo, int) else pl.multiple_of(lo, M), 2 * M if do_p else M)
        x_wait(2 * t - 1)
        if do_p:
            x_wait(2 * t)

        def tile(n, carry):
            slot = n % 2
            w_wait("gu", n, slot)

            @pl.when(n < nt - 1)
            def _():
                w_start("gu", n + 1, 1 - slot)

            @pl.when(n == nt - 1)
            def _():
                last_next()

            if isinstance(t, int) and t == 1:
                p_first(n, 0).wait()
                p_first(n, 1).wait()
            else:
                p_copy(t - 1, n).wait()
            for j in range(TN // SUB):
                cols = pl.ds(j * SUB, SUB)
                xv = xg[xrow, :]
                g = jnp.dot(xv, wring[slot, 0, :, cols], preferred_element_type=f32)
                u = jnp.dot(xv, wring[slot, 1, :, cols], preferred_element_type=f32)
                for k in range(2):
                    if do_p:
                        stage[n, pl.ds(k * M, HM), cols] = g[M + k * HM:M + (k + 1) * HM].astype(bf16)
                        stage[n, pl.ds(k * M + HM, HM), cols] = u[M + k * HM:M + (k + 1) * HM].astype(bf16)
                    og = g[k * HM:(k + 1) * HM] + recv[(t - 1) % 2, n, pl.ds(k * M, HM), cols].astype(f32)
                    ou = u[k * HM:(k + 1) * HM] + recv[(t - 1) % 2, n, pl.ds(k * M + HM, HM), cols].astype(f32)
                    h = og * jax.nn.sigmoid(og) * ou
                    hid[(t - 1) % 3, pl.ds(pl.multiple_of(a * M + k * HM, HM), HM),
                        pl.ds(pl.multiple_of(n * TN + j * SUB, SUB), SUB)] = h.astype(bf16)
            if do_p:
                p_copy(t, n).start()
            h_copy(t - 1, n, a).start()
            return carry

        lax.fori_loop(0, nt, tile, 0)

    def y_copy(s, q, h):
        cols = pl.ds(h * TN if isinstance(h, int) else pl.multiple_of(h * TN, TN), TN)
        dst = ymate.at[:, cols] if q == 1 else yrecv.at[s % 2, q // 2, :, cols]
        sem = ymsem.at[h] if q == 1 else yrsem.at[s % 2, q // 2, h]
        return pltpu.make_async_remote_copy(
            src_ref=ystage.at[q, :, cols], dst_ref=dst, send_sem=yssem.at[q, h], recv_sem=sem,
            device_id=(dp, a, mate(0 if q == 0 else 2)), device_id_type=MESH)

    def y_out(s, h):
        cols = pl.ds(h * TN, TN)
        return pltpu.make_async_copy(
            yout.at[:, cols], y_hbm.at[pl.ds(pl.multiple_of(s * 2 * M, 2 * M), 2 * M), cols], yosem.at[h])

    def finish(s, first):
        for h in range(per):
            for q in range(3):
                y_copy(s, q, h).wait_send()
            for q in (2, 0):
                y_copy(s, q, h).wait_recv()
            if first is not True:
                @pl.when(jnp.logical_not(first))
                def _():
                    y_out(s - 1, h).wait()

            def chunk(i, carry):
                r, cols = pl.ds(pl.multiple_of(i * 64, 64), 64), pl.ds(h * TN, TN)
                total = yown[r, cols] + yrecv[s % 2, 0, r, cols].astype(f32) + yrecv[s % 2, 1, r, cols].astype(f32)
                yout[r, cols] = total.astype(bf16)
                return carry

            lax.fori_loop(0, 2 * M // 64, chunk, 0)
            y_out(s, h).start()

    def arrived(s, lo, hi):
        def one(n, carry):
            h_copy(s, n, 1 - a).wait_recv()
            h_copy(s, n, a).wait_send()
            return carry

        lax.fori_loop(lo, hi, one, 0)

    def y_meet(q, h):
        @pl.when(q == 0)
        def _():
            y_copy(0, 1, h).wait_recv()

    def y_put(q, h, j, out):
        cols = pl.ds(pl.multiple_of(h * TN + j * SUB, SUB), SUB)

        @pl.when(q == 0)
        def _():
            ystage[0, :, cols] = (out + ymate[:, cols].astype(f32)).astype(bf16)

        @pl.when(jnp.logical_or(q == 1, q == 2))
        def _():
            ystage[q, :, cols] = out.astype(bf16)

        @pl.when(q == 3)
        def _():
            yown[:, cols] = out

    def y_send(s, q, h):
        for p in range(3):
            @pl.when(q == p)
            def _():
                y_copy(s, p, h).start()

    def down(s, last_next):
        arrived(s, 0, nt)

        def tile(i, carry):
            slot = i % 2
            q, h = d_tile(i)
            w_wait("d", i, slot)

            @pl.when(i < nd - 1)
            def _():
                w_start("d", i + 1, 1 - slot)

            @pl.when(i == nd - 1)
            def _():
                last_next()

            y_meet(q, h)
            for j in range(TN // SUB):
                wc = pl.ds(j * SUB, SUB)
                out = jnp.dot(hid[s % 3, :, pl.ds(0, half)], wring[slot, 0, pl.ds(0, half), wc],
                              preferred_element_type=f32)
                out = out + jnp.dot(hid[s % 3, :, pl.ds(half, half)], wring[slot, 1, pl.ds(0, half), wc],
                                    preferred_element_type=f32)
                y_put(q, h, j, out)
            y_send(s, q, h)
            return carry

        lax.fori_loop(0, nd, tile, 0)

    def down_last(s, p, between):
        arrived(s, p * (nt // 2), (p + 1) * (nt // 2))
        items = nd // 2

        def item(i, carry):
            slot = i % 2
            w_wait("d%d" % p, i, slot)

            @pl.when(i < items - 1)
            def _():
                w_start("d%d" % p, i + 1, 1 - slot)

            if p == 0:
                @pl.when(i == items - 1)
                def _():
                    w_start("d1", 0, 0)
                    between()

            for k in range(2):
                o = 2 * i + k
                q, h = d_tile(o)
                if p == 1:
                    y_meet(q, h)
                for j in range(TN // SUB):
                    wc = pl.ds(j * SUB, SUB)
                    out = jnp.dot(hid[s % 3, :, pl.ds(p * half, half)], wring[slot, k, pl.ds(0, half), wc],
                                  preferred_element_type=f32)
                    cols = pl.ds(k * TN + j * SUB, SUB)
                    if p == 0:
                        @pl.when(i < items - 1)
                        def _():
                            acc[i, :, cols] = out

                        @pl.when(i == items - 1)
                        def _():
                            yown[:, cols] = out
                    else:
                        @pl.when(i < items - 1)
                        def _():
                            y_put(q, h, j, acc[i, :, cols] + out)

                        @pl.when(i == items - 1)
                        def _():
                            yown[:, cols] = yown[:, cols] + out
                if p == 1:
                    y_send(s, q, h)
            return carry

        lax.fori_loop(0, items, item, 0)

    w_start("gu", 0, 0)
    for c in range(2 * steps):
        x_local(c).start()

    barrier = pltpu.get_barrier_semaphore()
    pl.semaphore_signal(barrier, inc=1, device_id=peer, device_id_type=MESH)
    for q in range(3):
        pl.semaphore_signal(barrier, inc=1, device_id=(dp, a, mate(q)), device_id_type=MESH)
    pl.semaphore_wait(barrier, 4)

    for q in range(2):
        for k in range(2):
            x_first(k, q).start()

    gu0 = lambda: w_start("gu", 0, 0)
    d0 = lambda: w_start("d", 0, 0)

    first(gu0)
    tiles(1, True, gu0)
    tiles(2, True, d0)
    down(0, gu0)

    def step(t, carry):
        tiles(t, True, d0)
        finish(t - 3, t == 3)
        down(t - 2, gu0)
        return carry

    lax.fori_loop(3, steps, step, 0)

    tiles(steps, False, d0)
    finish(steps - 3, steps == 3)
    down(steps - 2, lambda: w_start("d0", 0, 0))
    down_last(steps - 1, 0, lambda: finish(steps - 2, False))
    down_last(steps - 1, 1, None)
    finish(steps - 1, False)
    for h in range(per):
        y_out(steps - 1, h).wait()

    for k in range(2):
        for q in range(3):
            x_first(k, q).wait_send()

    def drain(c, carry):
        for q in range(3):
            x_remote(c, q).wait_send()
        return carry

    lax.fori_loop(1, 2 * steps, drain, 0)


def solution(mesh):
    def body(x, wg, wu, wd):
        rows, xcols = x.shape
        depth, ff = wg.shape
        dcols = wd.shape[1]
        steps, nt, per = rows // (2 * M), ff // TN, xcols // TN
        bf16 = jnp.bfloat16
        anyspace = pl.BlockSpec(memory_space=pl.ANY)
        dma = pltpu.SemaphoreType.DMA
        return pl.pallas_call(
            _kernel,
            out_shape=jax.ShapeDtypeStruct(x.shape, x.dtype),
            in_specs=[anyspace] * 4,
            out_specs=anyspace,
            scratch_shapes=[
                pltpu.VMEM((rows, depth), bf16),
                pltpu.VMEM((2, 2, depth, TN), bf16),
                pltpu.VMEM((nt, 2 * M, TN), bf16),
                pltpu.VMEM((2, nt, 2 * M, TN), bf16),
                pltpu.VMEM((3, 2 * M, ff), bf16),
                pltpu.VMEM((3, 2 * M, xcols), bf16),
                pltpu.VMEM((2, 2, 2 * M, xcols), bf16),
                pltpu.VMEM((2 * M, xcols), bf16),
                pltpu.VMEM((2 * M, xcols), jnp.float32),
                pltpu.VMEM((2 * M, xcols), bf16),
                pltpu.VMEM((dcols // (2 * TN) - 1, 2 * M, 2 * TN), jnp.float32),
                dma((2, 2)),
                dma((2 * steps,)),
                dma((2 * steps, 3)),
                dma((2 * steps, 3)),
                dma((3, 2)),
                dma((3, 2)),
                dma((nt,)),
                dma((2, nt)),
                dma((nt, 2)),
                dma((nt, 2)),
                dma((3, nt)),
                dma((3, nt)),
                dma((3, per)),
                dma((2, 2, per)),
                dma((per,)),
                dma((per,)),
            ],
            compiler_params=pltpu.CompilerParams(
                collective_id=0, has_side_effects=True, vmem_limit_bytes=67043328),
        )(x, wg, wu, wd)

    return jax.shard_map(
        body, mesh=mesh,
        in_specs=(P("dp", ("a", "b")), P("a", "b"), P("a", "b"), P("b", "a")),
        out_specs=P("dp", ("a", "b")), check_vma=False)
```

```python
import jax
import jax.numpy as jnp
from jax import lax
from jax.experimental import pallas as pl
from jax.experimental.pallas import tpu as pltpu
from jax.sharding import PartitionSpec as P

MESH = pl.DeviceIdType.MESH
M = 128
HM = M // 2
TN = 512
SUB = 512


def _kernel(x_hbm, wg_hbm, wu_hbm, wd_hbm, y_hbm,
            xg, wring, stage, recv, hid, ystage, yrecv, ymate, yown, yout, acc,
            wsem, xlsem, xssem, xrsem, x0ssem, x0rsem, pssem, prsem, p0ssem, p0rsem, hssem, hrsem, hlssem, hlrsem,
            yssem, yrsem, ymsem, yosem, ylssem, ylrsem, ylmsem, ylosem):
    f32, bf16 = jnp.float32, jnp.bfloat16
    rows, xcols = x_hbm.shape
    depth, ff = wg_hbm.shape
    dcols = wd_hbm.shape[1]
    half = ff // 2
    steps = rows // (2 * M)
    nt = ff // TN
    nd = dcols // TN
    per = xcols // TN

    dp = lax.axis_index("dp")
    a = lax.axis_index("a")
    b = lax.axis_index("b")
    chip, core = b // 2, b % 2
    peer = (dp, 1 - a, b)

    def mate(q):
        fx = 1 - q // 2
        fc = ((q + 1) // 2) % 2
        return 2 * (chip + fx - 2 * chip * fx) + core + fc - 2 * core * fc

    def d_tile(o):
        late = o // 4
        return (1 - late) * (1 - o % 2) + late * (o // 2), (1 - late) * (o // 2) + late * (o % 2)

    def w_copy(kind, i, slot, k):
        if kind == "gu":
            cols = pl.ds(pl.multiple_of(i * TN, TN), TN)
            return pltpu.make_async_copy((wg_hbm, wu_hbm)[k].at[:, cols], wring.at[slot, k], wsem.at[slot, k])
        q, h = d_tile(i if kind == "d" else 2 * i + k)
        part = {"d": k, "d0": 0, "d1": 1}[kind]
        cols = pl.ds(pl.multiple_of(mate(q) * xcols + h * TN, TN), TN)
        return pltpu.make_async_copy(
            wd_hbm.at[pl.ds(part * half, half), cols], wring.at[slot, k, pl.ds(0, half)], wsem.at[slot, k])

    def w_wait(kind, i, slot, k):
        w_copy(kind, i, slot, k).wait()

    def w_ahead(kind, i, count, then, slot, k):
        @pl.when(i < count - 2)
        def _():
            w_copy(kind, i + 2, slot, k).start()

        if then is not None:
            @pl.when(i >= count - 2)
            def _():
                w_copy(then, i + 2 - count, slot, k).start()

    def x_rows(c):
        s, mine = c // 2, c % 2
        src = s * 2 * M + (a * mine + (1 - a) * (1 - mine)) * M
        return pl.ds(pl.multiple_of(src, M), M), pl.ds(pl.multiple_of(c * M, M), M)

    def x_local(c):
        src, dst = x_rows(c)
        return pltpu.make_async_copy(
            x_hbm.at[src], xg.at[dst, pl.ds(pl.multiple_of(b * xcols, xcols), xcols)], xlsem.at[c])

    def x_remote(c, q):
        src, dst = x_rows(c)
        return pltpu.make_async_remote_copy(
            src_ref=x_hbm.at[src], dst_ref=xg.at[dst, pl.ds(pl.multiple_of(b * xcols, xcols), xcols)],
            send_sem=xssem.at[c, q], recv_sem=xrsem.at[c, q],
            device_id=(dp, a, mate(q)), device_id_type=MESH)

    def x_wait(c):
        x_local(c).wait()
        for q in range(3):
            x_remote(c, q).wait_recv()

    def x_first(k, q):
        src = pl.ds(pl.multiple_of((1 - a) * M + k * HM, HM), HM)
        dst = pl.ds(k * HM, HM)
        if q < 2:
            cols = pl.ds(pl.multiple_of(b * xcols, xcols), xcols)
            source = x_hbm.at[src]
        else:
            cols = pl.ds(pl.multiple_of(mate(0) * xcols, xcols), xcols)
            source = xg.at[dst, cols]
        return pltpu.make_async_remote_copy(
            src_ref=source, dst_ref=xg.at[dst, cols], send_sem=x0ssem.at[q, k], recv_sem=x0rsem.at[q, k],
            device_id=(dp, a, mate(0 if q == 0 else 2)), device_id_type=MESH)

    def p_first(n, k, z):
        ref = pl.ds(k * M + z * HM, HM)
        return pltpu.make_async_remote_copy(
            src_ref=stage.at[n, ref], dst_ref=recv.at[0, n, ref], send_sem=p0ssem.at[n, 2 * k + z],
            recv_sem=p0rsem.at[n, 2 * k + z], device_id=peer, device_id_type=MESH)

    def first(then):
        def tile(n, carry):
            slot = n % 2
            for k in range(2):
                @pl.when(n == 0)
                def _():
                    if k == 0:
                        x_local(0).wait()
                    x_first(k, 0).wait_recv()
                    x_first(k, 2).start()
                    x_first(k, 1).wait_recv()
                    x_first(k, 2).wait_recv()

                for z in range(2):
                    if k == 0:
                        w_wait("gu", n, slot, z)
                    for j in range(TN // SUB):
                        cols = pl.ds(j * SUB, SUB)
                        out = jnp.dot(xg[pl.ds(k * HM, HM), :], wring[slot, z, :, cols], preferred_element_type=f32)
                        stage[n, pl.ds(k * M + z * HM, HM), cols] = out.astype(bf16)
                    p_first(n, k, z).start()
                    if k == 1:
                        w_ahead("gu", n, nt, then, slot, z)

            for q in range(3):
                x_remote(n + 1, q).start()
            return carry

        lax.fori_loop(0, nt, tile, 0)
        for c in range(nt + 1, 2 * steps):
            for q in range(3):
                x_remote(c, q).start()

    def p_copy(t, n):
        return pltpu.make_async_remote_copy(
            src_ref=stage.at[n], dst_ref=recv.at[t % 2, n], send_sem=pssem.at[n], recv_sem=prsem.at[t % 2, n],
            device_id=peer, device_id_type=MESH)

    def h_copy(s, n, place):
        ref = hid.at[s % 3, pl.ds(pl.multiple_of(place * M, M), M), pl.ds(pl.multiple_of(n * TN, TN), TN)]
        return pltpu.make_async_remote_copy(
            src_ref=ref, dst_ref=ref, send_sem=hssem.at[s % 3, n], recv_sem=hrsem.at[s % 3, n],
            device_id=peer, device_id_type=MESH)

    def h_half(s, n, k, place):
        ref = hid.at[s % 3, pl.ds(pl.multiple_of(k * M + place * HM, HM), HM), pl.ds(pl.multiple_of(n * TN, TN), TN)]
        return pltpu.make_async_remote_copy(
            src_ref=ref, dst_ref=ref, send_sem=hlssem.at[n, k], recv_sem=hlrsem.at[n, k],
            device_id=peer, device_id_type=MESH)

    def tiles(t, do_p, then, p_late=False):
        lo = 2 * M * t - M
        xrow = pl.ds(lo if isinstance(lo, int) else pl.multiple_of(lo, M), 2 * M if do_p else M)
        x_wait(2 * t - 1)
        if do_p:
            x_wait(2 * t)

        def tile(n, carry):
            slot = n % 2
            if isinstance(t, int) and t == 1:
                for k in range(2):
                    for z in range(2):
                        p_first(n, k, z).wait()
            else:
                p_copy(t - 1, n).wait()
            for j in range(TN // SUB):
                cols = pl.ds(j * SUB, SUB)
                xv = xg[xrow, :]
                w_wait("gu", n, slot, 0)
                g = jnp.dot(xv, wring[slot, 0, :, cols], preferred_element_type=f32)
                w_ahead("gu", n, nt, then, slot, 0)
                w_wait("gu", n, slot, 1)
                u = jnp.dot(xv, wring[slot, 1, :, cols], preferred_element_type=f32)
                w_ahead("gu", n, nt, then, slot, 1)
                for k in range(2):
                    if do_p:
                        stage[n, pl.ds(k * M, HM), cols] = g[M + k * HM:M + (k + 1) * HM].astype(bf16)
                        stage[n, pl.ds(k * M + HM, HM), cols] = u[M + k * HM:M + (k + 1) * HM].astype(bf16)
                    og = g[k * HM:(k + 1) * HM] + recv[(t - 1) % 2, n, pl.ds(k * M, HM), cols].astype(f32)
                    ou = u[k * HM:(k + 1) * HM] + recv[(t - 1) % 2, n, pl.ds(k * M + HM, HM), cols].astype(f32)
                    h = og * jax.nn.sigmoid(og) * ou
                    hrow = a * M + k * HM if do_p else k * M + a * HM
                    hid[(t - 1) % 3, pl.ds(pl.multiple_of(hrow, HM), HM),
                        pl.ds(pl.multiple_of(n * TN + j * SUB, SUB), SUB)] = h.astype(bf16)
            if do_p and not p_late:
                p_copy(t, n).start()
            if do_p:
                h_copy(t - 1, n, a).start()
            else:
                h_half(t - 1, n, 0, a).start()
            return carry

        lax.fori_loop(0, nt, tile, 0)

        def after(n, carry):
            if do_p:
                p_copy(t, n).start()
            else:
                h_half(t - 1, n, 1, a).start()
            return carry

        if p_late or not do_p:
            lax.fori_loop(0, nt, after, 0)

    def y_copy(s, q, h, k=None):
        cols = pl.ds(h * TN if isinstance(h, int) else pl.multiple_of(h * TN, TN), TN)
        r = pl.ds(0, 2 * M) if k is None else pl.ds(k * M, M)
        dst = ymate.at[r, cols] if q == 1 else yrecv.at[s % 2, q // 2, r, cols]
        if k is None:
            send, sem = yssem.at[q, h], ymsem.at[h] if q == 1 else yrsem.at[s % 2, q // 2, h]
        else:
            send, sem = ylssem.at[q, h, k], ylmsem.at[h, k] if q == 1 else ylrsem.at[q // 2, h, k]
        return pltpu.make_async_remote_copy(
            src_ref=ystage.at[q, r, cols], dst_ref=dst, send_sem=send, recv_sem=sem,
            device_id=(dp, a, mate(0 if q == 0 else 2)), device_id_type=MESH)

    def y_out(s, h):
        cols = pl.ds(h * TN, TN)
        return pltpu.make_async_copy(
            yout.at[:, cols], y_hbm.at[pl.ds(pl.multiple_of(s * 2 * M, 2 * M), 2 * M), cols], yosem.at[h])

    def finish(s, first):
        for h in range(per):
            for q in range(3):
                y_copy(s, q, h).wait_send()
            for q in (2, 0):
                y_copy(s, q, h).wait_recv()
            if first is not True:
                @pl.when(jnp.logical_not(first))
                def _():
                    y_out(s - 1, h).wait()

            def chunk(i, carry):
                r, cols = pl.ds(pl.multiple_of(i * 64, 64), 64), pl.ds(h * TN, TN)
                total = yown[r, cols] + yrecv[s % 2, 0, r, cols].astype(f32) + yrecv[s % 2, 1, r, cols].astype(f32)
                yout[r, cols] = total.astype(bf16)
                return carry

            lax.fori_loop(0, 2 * M // 64, chunk, 0)
            y_out(s, h).start()

    def arrived(s, lo, hi):
        def one(n, carry):
            h_copy(s, n, 1 - a).wait_recv()
            h_copy(s, n, a).wait_send()
            return carry

        lax.fori_loop(lo, hi, one, 0)

    def y_meet(q, h, k=None):
        @pl.when(q == 0)
        def _():
            y_copy(0, 1, h, k).wait_recv()

    def y_put(q, h, j, out, k=None):
        cols = pl.ds(pl.multiple_of(h * TN + j * SUB, SUB), SUB)
        r = pl.ds(0, 2 * M) if k is None else pl.ds(k * M, M)

        @pl.when(q == 0)
        def _():
            ystage[0, r, cols] = (out + ymate[r, cols].astype(f32)).astype(bf16)

        @pl.when(jnp.logical_or(q == 1, q == 2))
        def _():
            ystage[q, r, cols] = out.astype(bf16)

        @pl.when(q == 3)
        def _():
            yown[r, cols] = out

    def y_send(s, q, h, k=None):
        for p in range(3):
            @pl.when(q == p)
            def _():
                y_copy(s, p, h, k).start()

    def down(s, then):
        arrived(s, 0, nt)

        def tile(i, carry):
            slot = i % 2
            q, h = d_tile(i)
            y_meet(q, h)
            w_wait("d", i, slot, 0)
            w_wait("d", i, slot, 1)
            out = jnp.dot(hid[s % 3, :, pl.ds(0, half)], wring[slot, 0, pl.ds(0, half)],
                          preferred_element_type=f32)
            out = out + jnp.dot(hid[s % 3, :, pl.ds(half, half)], wring[slot, 1, pl.ds(0, half)],
                                preferred_element_type=f32)
            y_put(q, h, 0, out)
            w_ahead("d", i, nd, then, slot, 0)
            w_ahead("d", i, nd, then, slot, 1)
            y_send(s, q, h)
            return carry

        lax.fori_loop(0, nd, tile, 0)

    def y_out_last(s, k, h, place):
        cols = pl.ds(h * TN, TN)
        return pltpu.make_async_copy(
            yout.at[pl.ds(k * M + place * HM, HM), cols],
            y_hbm.at[pl.ds(s * 2 * M + place * M + k * HM, HM), cols], ylosem.at[k, h, place])

    def finish_last(s, k):
        for h in range(per):
            for q in range(3):
                y_copy(s, q, h, k).wait_send()
            for q in (2, 0):
                y_copy(s, q, h, k).wait_recv()
            if k == 0:
                y_out(s - 1, h).wait()
            r, cols = pl.ds(k * M, M), pl.ds(h * TN, TN)
            total = yown[r, cols] + yrecv[s % 2, 0, r, cols].astype(f32) + yrecv[s % 2, 1, r, cols].astype(f32)
            yout[r, cols] = total.astype(bf16)
            for place in range(2):
                y_out_last(s, k, h, place).start()

    def down_last(s, k, p, then):
        def one(n, carry):
            h_half(s, n, k, 1 - a).wait_recv()
            h_half(s, n, k, a).wait_send()
            return carry

        lax.fori_loop(p * (nt // 2), (p + 1) * (nt // 2), one, 0)
        items = nd // 2

        def item(i, carry):
            slot = i % 2
            r = pl.ds(k * M, M)
            for e in range(2):
                q, h = d_tile(2 * i + e)
                if p == 1:
                    y_meet(q, h, k)
                w_wait("d%d" % p, i, slot, e)
                for j in range(TN // SUB):
                    wc = pl.ds(j * SUB, SUB)
                    out = jnp.dot(hid[s % 3, r, pl.ds(p * half, half)], wring[slot, e, pl.ds(0, half), wc],
                                  preferred_element_type=f32)
                    cols = pl.ds(e * TN + j * SUB, SUB)
                    if p == 0:
                        acc[i, :, cols] = out
                    else:
                        y_put(q, h, j, acc[i, :, cols] + out, k)
                w_ahead("d%d" % p, i, items, then, slot, e)
                if p == 1:
                    y_send(s, q, h, k)
            return carry

        lax.fori_loop(0, items, item, 0)

    for i in range(2):
        for k in range(2):
            w_copy("gu", i, i, k).start()
    for c in range(2 * steps):
        x_local(c).start()

    barrier = pltpu.get_barrier_semaphore()
    pl.semaphore_signal(barrier, inc=1, device_id=peer, device_id_type=MESH)
    for q in range(3):
        pl.semaphore_signal(barrier, inc=1, device_id=(dp, a, mate(q)), device_id_type=MESH)
    pl.semaphore_wait(barrier, 4)

    for q in range(2):
        for k in range(2):
            x_first(k, q).start()

    first("gu")
    tiles(1, True, "gu")
    tiles(2, True, "d")
    down(0, "gu")

    def step(t, carry):
        tiles(t, True, "d")
        finish(t - 3, t == 3)
        down(t - 2, "gu")
        return carry

    last = steps - 1
    lax.fori_loop(3, last, step, 0)

    tiles(last, True, "d", p_late=True)
    finish(last - 3, False)
    down(last - 2, "d")
    finish(last - 2, False)
    down(last - 1, "gu")
    tiles(steps, False, "d0")
    finish(last - 1, False)
    down_last(last, 0, 0, "d1")
    down_last(last, 0, 1, "d0")
    down_last(last, 1, 0, "d1")
    finish_last(last, 0)
    down_last(last, 1, 1, None)
    finish_last(last, 1)
    for k in range(2):
        for h in range(per):
            for place in range(2):
                y_out_last(last, k, h, place).wait()

    for k in range(2):
        for q in range(3):
            x_first(k, q).wait_send()

    def drain(c, carry):
        for q in range(3):
            x_remote(c, q).wait_send()
        return carry

    lax.fori_loop(1, 2 * steps, drain, 0)


def solution(mesh):
    def body(x, wg, wu, wd):
        rows, xcols = x.shape
        depth, ff = wg.shape
        dcols = wd.shape[1]
        steps, nt, per = rows // (2 * M), ff // TN, xcols // TN
        bf16 = jnp.bfloat16
        anyspace = pl.BlockSpec(memory_space=pl.ANY)
        dma = pltpu.SemaphoreType.DMA
        return pl.pallas_call(
            _kernel,
            out_shape=jax.ShapeDtypeStruct(x.shape, x.dtype),
            in_specs=[anyspace] * 4,
            out_specs=anyspace,
            scratch_shapes=[
                pltpu.VMEM((rows, depth), bf16),
                pltpu.VMEM((2, 2, depth, TN), bf16),
                pltpu.VMEM((nt, 2 * M, TN), bf16),
                pltpu.VMEM((2, nt, 2 * M, TN), bf16),
                pltpu.VMEM((3, 2 * M, ff), bf16),
                pltpu.VMEM((3, 2 * M, xcols), bf16),
                pltpu.VMEM((2, 2, 2 * M, xcols), bf16),
                pltpu.VMEM((2 * M, xcols), bf16),
                pltpu.VMEM((2 * M, xcols), jnp.float32),
                pltpu.VMEM((2 * M, xcols), bf16),
                pltpu.VMEM((dcols // (2 * TN), M, 2 * TN), jnp.float32),
                dma((2, 2)),
                dma((2 * steps,)),
                dma((2 * steps, 3)),
                dma((2 * steps, 3)),
                dma((3, 2)),
                dma((3, 2)),
                dma((nt,)),
                dma((2, nt)),
                dma((nt, 4)),
                dma((nt, 4)),
                dma((3, nt)),
                dma((3, nt)),
                dma((nt, 2)),
                dma((nt, 2)),
                dma((3, per)),
                dma((2, 2, per)),
                dma((per,)),
                dma((per,)),
                dma((3, per, 2)),
                dma((2, per, 2)),
                dma((per, 2)),
                dma((2, per, 2)),
            ],
            compiler_params=pltpu.CompilerParams(
                collective_id=0, has_side_effects=True, vmem_limit_bytes=67043328),
        )(x, wg, wu, wd)

    return jax.shard_map(
        body, mesh=mesh,
        in_specs=(P("dp", ("a", "b")), P("a", "b"), P("a", "b"), P("b", "a")),
        out_specs=P("dp", ("a", "b")), check_vma=False)
```

```python
import jax
import jax.numpy as jnp
from jax import lax
from jax.experimental import pallas as pl
from jax.experimental.pallas import tpu as pltpu
from jax.sharding import PartitionSpec as P

MESH = pl.DeviceIdType.MESH
M = 128
HM = M // 2
TN = 512
SUB = 512


def _kernel(x_hbm, wg_hbm, wu_hbm, wd_hbm, y_hbm,
            xg, wring, stage, recv, hid, ystage, yrecv, ymate, yown, yout, acc,
            wsem, xlsem, xssem, xrsem, x0ssem, x0rsem, pssem, prsem, p0ssem, p0rsem, hssem, hrsem, hlssem, hlrsem,
            yssem, yrsem, ymsem, yosem, ylssem, ylrsem, ylmsem, ylosem):
    f32, bf16 = jnp.float32, jnp.bfloat16
    rows, xcols = x_hbm.shape
    depth, ff = wg_hbm.shape
    dcols = wd_hbm.shape[1]
    half = ff // 2
    steps = rows // (2 * M)
    nt = ff // TN
    nd = dcols // TN
    per = xcols // TN

    dp = lax.axis_index("dp")
    a = lax.axis_index("a")
    b = lax.axis_index("b")
    chip, core = b // 2, b % 2
    peer = (dp, 1 - a, b)

    def mate(q):
        fx = 1 - q // 2
        fc = ((q + 1) // 2) % 2
        return 2 * (chip + fx - 2 * chip * fx) + core + fc - 2 * core * fc

    def d_tile(o):
        late = o // 4
        return (1 - late) * (1 - o % 2) + late * (o // 2), (1 - late) * (o // 2) + late * (o % 2)

    def w_copy(kind, i, slot, k):
        if kind == "gu":
            cols = pl.ds(pl.multiple_of(i * TN, TN), TN)
            return pltpu.make_async_copy((wg_hbm, wu_hbm)[k].at[:, cols], wring.at[slot, k], wsem.at[slot, k])
        q, h = d_tile(i if kind == "d" else 2 * i + k)
        part = {"d": k, "d0": 0, "d1": 1}[kind]
        cols = pl.ds(pl.multiple_of(mate(q) * xcols + h * TN, TN), TN)
        return pltpu.make_async_copy(
            wd_hbm.at[pl.ds(part * half, half), cols], wring.at[slot, k, pl.ds(0, half)], wsem.at[slot, k])

    def w_wait(kind, i, slot, k):
        w_copy(kind, i, slot, k).wait()

    def w_ahead(kind, i, count, then, slot, k):
        @pl.when(i < count - 2)
        def _():
            w_copy(kind, i + 2, slot, k).start()

        if then is not None:
            @pl.when(i >= count - 2)
            def _():
                w_copy(then, i + 2 - count, slot, k).start()

    def x_rows(c):
        s, mine = c // 2, c % 2
        src = s * 2 * M + (a * mine + (1 - a) * (1 - mine)) * M
        return pl.ds(pl.multiple_of(src, M), M), pl.ds(pl.multiple_of(c * M, M), M)

    def x_local(c):
        src, dst = x_rows(c)
        return pltpu.make_async_copy(
            x_hbm.at[src], xg.at[dst, pl.ds(pl.multiple_of(b * xcols, xcols), xcols)], xlsem.at[c])

    def x_remote(c, q):
        src, dst = x_rows(c)
        return pltpu.make_async_remote_copy(
            src_ref=x_hbm.at[src], dst_ref=xg.at[dst, pl.ds(pl.multiple_of(b * xcols, xcols), xcols)],
            send_sem=xssem.at[c, q], recv_sem=xrsem.at[c, q],
            device_id=(dp, a, mate(q)), device_id_type=MESH)

    def x_wait(c):
        x_local(c).wait()
        for q in range(3):
            x_remote(c, q).wait_recv()

    def x_first(k, q):
        src = pl.ds(pl.multiple_of((1 - a) * M + k * HM, HM), HM)
        dst = pl.ds(k * HM, HM)
        if q < 2:
            cols = pl.ds(pl.multiple_of(b * xcols, xcols), xcols)
            source = x_hbm.at[src]
        else:
            cols = pl.ds(pl.multiple_of(mate(0) * xcols, xcols), xcols)
            source = xg.at[dst, cols]
        return pltpu.make_async_remote_copy(
            src_ref=source, dst_ref=xg.at[dst, cols], send_sem=x0ssem.at[q, k], recv_sem=x0rsem.at[q, k],
            device_id=(dp, a, mate(0 if q == 0 else 2)), device_id_type=MESH)

    def p_first(n, k, z):
        ref = pl.ds(k * M + z * HM, HM)
        return pltpu.make_async_remote_copy(
            src_ref=stage.at[n, ref], dst_ref=recv.at[0, n, ref], send_sem=p0ssem.at[n, 2 * k + z],
            recv_sem=p0rsem.at[n, 2 * k + z], device_id=peer, device_id_type=MESH)

    def first(then):
        def tile(n, carry):
            slot = n % 2
            for k in range(2):
                @pl.when(n == 0)
                def _():
                    if k == 0:
                        x_local(0).wait()
                    x_first(k, 0).wait_recv()
                    x_first(k, 2).start()
                    x_first(k, 1).wait_recv()
                    x_first(k, 2).wait_recv()

                for z in range(2):
                    if k == 0:
                        w_wait("gu", n, slot, z)
                    for j in range(TN // SUB):
                        cols = pl.ds(j * SUB, SUB)
                        out = jnp.dot(xg[pl.ds(k * HM, HM), :], wring[slot, z, :, cols], preferred_element_type=f32)
                        stage[n, pl.ds(k * M + z * HM, HM), cols] = out.astype(bf16)
                    p_first(n, k, z).start()
                    if k == 1:
                        w_ahead("gu", n, nt, then, slot, z)

            for q in range(3):
                x_remote(n + 1, q).start()
            return carry

        lax.fori_loop(0, nt, tile, 0)
        for c in range(nt + 1, 2 * steps):
            for q in range(3):
                x_remote(c, q).start()

    def p_copy(t, m):
        pair = pl.ds(2 * m, 2)
        return pltpu.make_async_remote_copy(
            src_ref=stage.at[pair], dst_ref=recv.at[t % 2, pair], send_sem=pssem.at[m], recv_sem=prsem.at[t % 2, m],
            device_id=peer, device_id_type=MESH)

    def h_copy(s, m, place):
        ref = hid.at[s % 3, pl.ds(pl.multiple_of(place * M, M), M), pl.ds(pl.multiple_of(m * 2 * TN, 2 * TN), 2 * TN)]
        return pltpu.make_async_remote_copy(
            src_ref=ref, dst_ref=ref, send_sem=hssem.at[s % 3, m], recv_sem=hrsem.at[s % 3, m],
            device_id=peer, device_id_type=MESH)

    def h_half(s, n, k, place):
        ref = hid.at[s % 3, pl.ds(pl.multiple_of(k * M + place * HM, HM), HM), pl.ds(pl.multiple_of(n * TN, TN), TN)]
        return pltpu.make_async_remote_copy(
            src_ref=ref, dst_ref=ref, send_sem=hlssem.at[n, k], recv_sem=hlrsem.at[n, k],
            device_id=peer, device_id_type=MESH)

    def tiles(t, do_p, then, p_late=False):
        lo = 2 * M * t - M
        xrow = pl.ds(lo if isinstance(lo, int) else pl.multiple_of(lo, M), 2 * M if do_p else M)
        x_wait(2 * t - 1)
        if do_p:
            x_wait(2 * t)

        def tile(n, carry):
            slot = n % 2
            if isinstance(t, int) and t == 1:
                for k in range(2):
                    for z in range(2):
                        p_first(n, k, z).wait()
            else:
                @pl.when(n % 2 == 0)
                def _():
                    p_copy(t - 1, n // 2).wait()
            for j in range(TN // SUB):
                cols = pl.ds(j * SUB, SUB)
                xv = xg[xrow, :]
                w_wait("gu", n, slot, 0)
                g = jnp.dot(xv, wring[slot, 0, :, cols], preferred_element_type=f32)
                w_ahead("gu", n, nt, then, slot, 0)
                w_wait("gu", n, slot, 1)
                u = jnp.dot(xv, wring[slot, 1, :, cols], preferred_element_type=f32)
                w_ahead("gu", n, nt, then, slot, 1)
                for k in range(2):
                    if do_p:
                        stage[n, pl.ds(k * M, HM), cols] = g[M + k * HM:M + (k + 1) * HM].astype(bf16)
                        stage[n, pl.ds(k * M + HM, HM), cols] = u[M + k * HM:M + (k + 1) * HM].astype(bf16)
                    og = g[k * HM:(k + 1) * HM] + recv[(t - 1) % 2, n, pl.ds(k * M, HM), cols].astype(f32)
                    ou = u[k * HM:(k + 1) * HM] + recv[(t - 1) % 2, n, pl.ds(k * M + HM, HM), cols].astype(f32)
                    h = og * jax.nn.sigmoid(og) * ou
                    hrow = a * M + k * HM if do_p else k * M + a * HM
                    hid[(t - 1) % 3, pl.ds(pl.multiple_of(hrow, HM), HM),
                        pl.ds(pl.multiple_of(n * TN + j * SUB, SUB), SUB)] = h.astype(bf16)
            if do_p:
                @pl.when(n % 2 == 1)
                def _():
                    if not p_late:
                        p_copy(t, n // 2).start()
                    h_copy(t - 1, n // 2, a).start()
            else:
                h_half(t - 1, n, 0, a).start()
            return carry

        lax.fori_loop(0, nt, tile, 0)

        def after(n, carry):
            if do_p:
                p_copy(t, n).start()
            else:
                h_half(t - 1, n, 1, a).start()
            return carry

        if p_late or not do_p:
            lax.fori_loop(0, nt // 2 if do_p else nt, after, 0)

    def y_copy(s, q, h, k=None):
        cols = pl.ds(h * TN if isinstance(h, int) else pl.multiple_of(h * TN, TN), TN)
        r = pl.ds(0, 2 * M) if k is None else pl.ds(k * M, M)
        dst = ymate.at[r, cols] if q == 1 else yrecv.at[s % 2, q // 2, r, cols]
        if k is None:
            send, sem = yssem.at[q, h], ymsem.at[h] if q == 1 else yrsem.at[s % 2, q // 2, h]
        else:
            send, sem = ylssem.at[q, h, k], ylmsem.at[h, k] if q == 1 else ylrsem.at[q // 2, h, k]
        return pltpu.make_async_remote_copy(
            src_ref=ystage.at[q, r, cols], dst_ref=dst, send_sem=send, recv_sem=sem,
            device_id=(dp, a, mate(0 if q == 0 else 2)), device_id_type=MESH)

    def y_out(s, h):
        cols = pl.ds(h * TN, TN)
        return pltpu.make_async_copy(
            yout.at[:, cols], y_hbm.at[pl.ds(pl.multiple_of(s * 2 * M, 2 * M), 2 * M), cols], yosem.at[h])

    def finish(s, first):
        for h in range(per):
            for q in range(3):
                y_copy(s, q, h).wait_send()
            for q in (2, 0):
                y_copy(s, q, h).wait_recv()
            if first is not True:
                @pl.when(jnp.logical_not(first))
                def _():
                    y_out(s - 1, h).wait()

            def chunk(i, carry):
                r, cols = pl.ds(pl.multiple_of(i * 64, 64), 64), pl.ds(h * TN, TN)
                total = yown[r, cols] + yrecv[s % 2, 0, r, cols].astype(f32) + yrecv[s % 2, 1, r, cols].astype(f32)
                yout[r, cols] = total.astype(bf16)
                return carry

            lax.fori_loop(0, 2 * M // 64, chunk, 0)
            y_out(s, h).start()

    def arrived(s):
        def one(m, carry):
            h_copy(s, m, 1 - a).wait_recv()
            h_copy(s, m, a).wait_send()
            return carry

        lax.fori_loop(0, nt // 2, one, 0)

    def y_meet(q, h, k=None):
        @pl.when(q == 0)
        def _():
            y_copy(0, 1, h, k).wait_recv()

    def y_put(q, h, j, out, k=None):
        cols = pl.ds(pl.multiple_of(h * TN + j * SUB, SUB), SUB)
        r = pl.ds(0, 2 * M) if k is None else pl.ds(k * M, M)

        @pl.when(q == 0)
        def _():
            ystage[0, r, cols] = (out + ymate[r, cols].astype(f32)).astype(bf16)

        @pl.when(jnp.logical_or(q == 1, q == 2))
        def _():
            ystage[q, r, cols] = out.astype(bf16)

        @pl.when(q == 3)
        def _():
            yown[r, cols] = out

    def y_send(s, q, h, k=None):
        for p in range(3):
            @pl.when(q == p)
            def _():
                y_copy(s, p, h, k).start()

    def down(s, then):
        arrived(s)

        def tile(i, carry):
            slot = i % 2
            q, h = d_tile(i)
            y_meet(q, h)
            w_wait("d", i, slot, 0)
            w_wait("d", i, slot, 1)
            out = jnp.dot(hid[s % 3, :, pl.ds(0, half)], wring[slot, 0, pl.ds(0, half)],
                          preferred_element_type=f32)
            out = out + jnp.dot(hid[s % 3, :, pl.ds(half, half)], wring[slot, 1, pl.ds(0, half)],
                                preferred_element_type=f32)
            y_put(q, h, 0, out)
            w_ahead("d", i, nd, then, slot, 0)
            w_ahead("d", i, nd, then, slot, 1)
            y_send(s, q, h)
            return carry

        lax.fori_loop(0, nd, tile, 0)

    def y_out_last(s, k, h, place):
        cols = pl.ds(h * TN, TN)
        return pltpu.make_async_copy(
            yout.at[pl.ds(k * M + place * HM, HM), cols],
            y_hbm.at[pl.ds(s * 2 * M + place * M + k * HM, HM), cols], ylosem.at[k, h, place])

    def finish_last(s, k):
        for h in range(per):
            for q in range(3):
                y_copy(s, q, h, k).wait_send()
            for q in (2, 0):
                y_copy(s, q, h, k).wait_recv()
            if k == 0:
                y_out(s - 1, h).wait()
            r, cols = pl.ds(k * M, M), pl.ds(h * TN, TN)
            total = yown[r, cols] + yrecv[s % 2, 0, r, cols].astype(f32) + yrecv[s % 2, 1, r, cols].astype(f32)
            yout[r, cols] = total.astype(bf16)
            for place in range(2):
                y_out_last(s, k, h, place).start()

    def down_last(s, k, p, then):
        def one(n, carry):
            h_half(s, n, k, 1 - a).wait_recv()
            h_half(s, n, k, a).wait_send()
            return carry

        lax.fori_loop(p * (nt // 2), (p + 1) * (nt // 2), one, 0)
        items = nd // 2

        def item(i, carry):
            slot = i % 2
            r = pl.ds(k * M, M)
            for e in range(2):
                q, h = d_tile(2 * i + e)
                if p == 1:
                    y_meet(q, h, k)
                w_wait("d%d" % p, i, slot, e)
                for j in range(TN // SUB):
                    wc = pl.ds(j * SUB, SUB)
                    out = jnp.dot(hid[s % 3, r, pl.ds(p * half, half)], wring[slot, e, pl.ds(0, half), wc],
                                  preferred_element_type=f32)
                    cols = pl.ds(e * TN + j * SUB, SUB)
                    if p == 0:
                        acc[i, :, cols] = out
                    else:
                        y_put(q, h, j, acc[i, :, cols] + out, k)
                w_ahead("d%d" % p, i, items, then, slot, e)
                if p == 1:
                    y_send(s, q, h, k)
            return carry

        lax.fori_loop(0, items, item, 0)

    for i in range(2):
        for k in range(2):
            w_copy("gu", i, i, k).start()
    for c in range(2 * steps):
        x_local(c).start()

    barrier = pltpu.get_barrier_semaphore()
    pl.semaphore_signal(barrier, inc=1, device_id=peer, device_id_type=MESH)
    for q in range(3):
        pl.semaphore_signal(barrier, inc=1, device_id=(dp, a, mate(q)), device_id_type=MESH)
    pl.semaphore_wait(barrier, 4)

    for q in range(2):
        for k in range(2):
            x_first(k, q).start()

    first("gu")
    tiles(1, True, "gu")
    tiles(2, True, "d")
    down(0, "gu")

    def step(t, carry):
        tiles(t, True, "d")
        finish(t - 3, t == 3)
        down(t - 2, "gu")
        return carry

    last = steps - 1
    lax.fori_loop(3, last, step, 0)

    tiles(last, True, "d", p_late=True)
    finish(last - 3, False)
    down(last - 2, "d")
    finish(last - 2, False)
    down(last - 1, "gu")
    tiles(steps, False, "d0")
    finish(last - 1, False)
    down_last(last, 0, 0, "d1")
    down_last(last, 0, 1, "d0")
    down_last(last, 1, 0, "d1")
    finish_last(last, 0)
    down_last(last, 1, 1, None)
    finish_last(last, 1)
    for k in range(2):
        for h in range(per):
            for place in range(2):
                y_out_last(last, k, h, place).wait()

    for k in range(2):
        for q in range(3):
            x_first(k, q).wait_send()

    def drain(c, carry):
        for q in range(3):
            x_remote(c, q).wait_send()
        return carry

    lax.fori_loop(1, 2 * steps, drain, 0)


def solution(mesh):
    def body(x, wg, wu, wd):
        rows, xcols = x.shape
        depth, ff = wg.shape
        dcols = wd.shape[1]
        steps, nt, per = rows // (2 * M), ff // TN, xcols // TN
        bf16 = jnp.bfloat16
        anyspace = pl.BlockSpec(memory_space=pl.ANY)
        dma = pltpu.SemaphoreType.DMA
        return pl.pallas_call(
            _kernel,
            out_shape=jax.ShapeDtypeStruct(x.shape, x.dtype),
            in_specs=[anyspace] * 4,
            out_specs=anyspace,
            scratch_shapes=[
                pltpu.VMEM((rows, depth), bf16),
                pltpu.VMEM((2, 2, depth, TN), bf16),
                pltpu.VMEM((nt, 2 * M, TN), bf16),
                pltpu.VMEM((2, nt, 2 * M, TN), bf16),
                pltpu.VMEM((3, 2 * M, ff), bf16),
                pltpu.VMEM((3, 2 * M, xcols), bf16),
                pltpu.VMEM((2, 2, 2 * M, xcols), bf16),
                pltpu.VMEM((2 * M, xcols), bf16),
                pltpu.VMEM((2 * M, xcols), jnp.float32),
                pltpu.VMEM((2 * M, xcols), bf16),
                pltpu.VMEM((dcols // (2 * TN), M, 2 * TN), jnp.float32),
                dma((2, 2)),
                dma((2 * steps,)),
                dma((2 * steps, 3)),
                dma((2 * steps, 3)),
                dma((3, 2)),
                dma((3, 2)),
                dma((nt // 2,)),
                dma((2, nt // 2)),
                dma((nt, 4)),
                dma((nt, 4)),
                dma((3, nt // 2)),
                dma((3, nt // 2)),
                dma((nt, 2)),
                dma((nt, 2)),
                dma((3, per)),
                dma((2, 2, per)),
                dma((per,)),
                dma((per,)),
                dma((3, per, 2)),
                dma((2, per, 2)),
                dma((per, 2)),
                dma((2, per, 2)),
            ],
            compiler_params=pltpu.CompilerParams(
                collective_id=0, has_side_effects=True, vmem_limit_bytes=67043328),
        )(x, wg, wu, wd)

    return jax.shard_map(
        body, mesh=mesh,
        in_specs=(P("dp", ("a", "b")), P("a", "b"), P("a", "b"), P("b", "a")),
        out_specs=P("dp", ("a", "b")), check_vma=False)
```
